32 devices in a mesh: dp: 4 (over z), vocab: 8 (over y, x, core).
Axes of the slice: x: 2, y: 2, z: 4, core: 2. Of those that a mesh axis runs over, the one named last changes fastest.
Arguments:
- teacher_logits: bfloat16 [1536, 151552], P('dp', 'vocab'), may hold values from -40 to 320, as said below
- student_logits: bfloat16 [1536, 126976], P('dp', 'vocab'), may hold values from -40 to 320, as said below
- tile_dest: int32 [1184, 2], replicated, may hold values from 0 to 991, as said below
- tile_weight: bfloat16 [1184, 2, 128, 128], P('vocab'), may hold values from 0.0009994507 to 1
- token_mask: int32 [1536], P('dp'), may hold values from 0 to 1, as said below
Outputs:
- token_loss: float32 [1536], P('dp')
- mean_loss: float32 [], replicated
The draws below stay inside these ranges and needn't reach their ends.
Inputs may be any that keep to these rules, and one draw needn't show every extreme that they name: `teacher_logits`: Real-valued logits. `student_logits`: Real-valued logits. `tile_dest`: row b names the student blocks of the 2 tiles of teacher block b. Student block s belongs to vocab index s // 124, teacher block b to vocab index b // 148. Of the tiles of the teacher blocks of one vocab index, at most 37 name student blocks of any one vocab index, and exactly 37 do for some vocab index. `token_mask`: at least one token has a 1.
All inputs are finite; a program needn't handle non-finite values.
Results may differ from the reference program's by a relative error of at most 0.0031.
Values may be sent and summed in bfloat16 or wider, within the bound.
A program may use at most 192 MiB of HBM per device.

```python
import math
import jax
import jax.numpy as jnp
from jax import lax

BLOCK = 128
VT = 151552
VS = 126976
K = 2
TOKENS = 1536
TBLOCKS = 1184
SBLOCKS = 992
TB_DEV = 148
SB_DEV = 124
CAP = 37
N_VOCAB = 8


def logit_field(key, row_count, col_count):
    key_base = jax.random.fold_in(key, 0)
    base_vals = jnp.clip(3.0 * jax.random.normal(key_base, (row_count, col_count), jnp.float32), -12.0, 12.0)
    return base_vals


def draw_teacher_logits(key, part):
    return logit_field(jax.random.fold_in(key, 11), TOKENS, VT).astype(jnp.bfloat16)


def draw_student_logits(key, part):
    return logit_field(jax.random.fold_in(key, 17), TOKENS, VS).astype(jnp.bfloat16)


def draw_tile_dest(key, part):
    tile_count = TB_DEV * K
    slot_count = N_VOCAB * CAP

    def one_source(source):
        sub_key = jax.random.fold_in(jax.random.fold_in(key, 29), source)
        key_score, key_pick, key_local = jax.random.split(sub_key, 3)
        position = jnp.arange(slot_count, dtype=jnp.int32)
        scores = jax.random.randint(key_score, (slot_count,), 0, 2 ** 20) * slot_count + position
        chosen = jax.random.randint(key_pick, (), 0, N_VOCAB)
        scores = jnp.where(position // CAP == chosen, scores - 2 ** 30, scores)
        slot_order = jnp.argsort(scores, stable=True)[:tile_count]
        owners = slot_order // CAP
        local_block = jax.random.randint(key_local, (tile_count,), 0, SB_DEV)
        return (owners * SB_DEV + local_block).astype(jnp.int32)
    sources = jax.vmap(one_source)(jnp.arange(N_VOCAB, dtype=jnp.int32))
    return sources.reshape(TBLOCKS, K)


def draw_token_mask(key, part):
    key_bits, key_keep = jax.random.split(jax.random.fold_in(key, 43))
    mask_vals = (jax.random.randint(key_bits, (TOKENS,), 0, 4) > 0).astype(jnp.int32)
    kept = jax.random.randint(key_keep, (), 0, TOKENS)
    position = jnp.arange(TOKENS, dtype=jnp.int32)
    return jnp.where(position == kept, 1, mask_vals).astype(jnp.int32)


def block_levels(stream_key, extent, pieces, smallest, largest):
    def one(dim, shards_of):
        heights = jax.random.uniform(jax.random.fold_in(jax.random.fold_in(stream_key, 6), dim), (shards_of,), jnp.float32, smallest / len(pieces), largest / len(pieces))
        return jnp.repeat(jnp.exp(heights), extent[dim] // shards_of).reshape((-1,) + (1,) * (len(extent) - dim - 1))

    loudness = one(*pieces[0])
    for cut in pieces[1:]:
        loudness = loudness * one(*cut)
    return loudness


def setup_inputs(seed: int = 0) -> dict:
    streams_of = jax.random.split(jax.random.key(seed), 6)
    return {
        "teacher_logits": draw_teacher_logits(jax.random.fold_in(streams_of[5], 71), 0),
        "student_logits": draw_student_logits(jax.random.fold_in(streams_of[5], 71), 0),
        "tile_dest": draw_tile_dest(jax.random.fold_in(streams_of[5], 71), 0),
        "tile_weight": jnp.clip(jnp.exp(math.log(1.0) - 6.9083047 * jax.random.uniform(streams_of[3], (TBLOCKS, K, BLOCK, BLOCK), jnp.float32) ** block_levels(streams_of[3], (TBLOCKS, K, BLOCK, BLOCK), ((0, 8),), -0.2, 0.2)), 0.0009994507, 1.0).astype(jnp.bfloat16),
        "token_mask": draw_token_mask(jax.random.fold_in(streams_of[5], 71), 0),
    }


SMOOTH = 0.1


def reference(teacher_logits, student_logits, tile_dest, tile_weight, token_mask):
    weights = tile_weight.astype(jnp.float32)
    mapping = (weights / jnp.sum(weights, axis=(1, 3), keepdims=True)).astype(jnp.bfloat16)
    mapping = lax.optimization_barrier(mapping).astype(jnp.float32)
    targets = tile_dest.reshape(-1).astype(jnp.int32)
    row_count = math.gcd(TOKENS, 256)

    def one_block(block_args):
        teacher_vals, student_vals, mask_vals = block_args
        teacher_vals = teacher_vals.astype(jnp.float32)
        maximum = jnp.max(teacher_vals, axis=1, keepdims=True)
        expon = jnp.exp(teacher_vals - maximum)
        teacher_prob = (expon / jnp.sum(expon, axis=1, keepdims=True)).astype(jnp.bfloat16)
        teacher_prob = lax.optimization_barrier(teacher_prob).astype(jnp.float32)
        prob_blocks = teacher_prob.reshape(row_count, TBLOCKS, BLOCK)
        partial_value = jnp.einsum('rbc,bkcd->bkrd', prob_blocks, mapping)
        partial_value = lax.optimization_barrier(partial_value.astype(jnp.bfloat16)).astype(jnp.float32)
        summed = jax.ops.segment_sum(partial_value.reshape(TBLOCKS * K, row_count, BLOCK), targets, num_segments=SBLOCKS)
        mapped = jnp.transpose(summed, (1, 0, 2)).reshape(row_count, VS)
        target = (1.0 - SMOOTH) * mapped + SMOOTH / VS
        student_vals = student_vals.astype(jnp.float32)
        student_max = jnp.max(student_vals, axis=1, keepdims=True)
        student_sum = jnp.sum(jnp.exp(student_vals - student_max), axis=1, keepdims=True)
        student_logp = student_vals - student_max - jnp.log(student_sum)
        token_kl = jnp.sum(target * (jnp.log(target) - student_logp), axis=1)
        return mask_vals.astype(jnp.float32) * token_kl

    token_loss = lax.map(one_block, (teacher_logits.reshape(-1, row_count, VT), student_logits.reshape(-1, row_count, VS), token_mask.reshape(-1, row_count)))
    token_loss = token_loss.reshape(TOKENS)
    counted = jnp.sum(token_mask.astype(jnp.float32))
    mean_loss = jnp.sum(token_loss) / counted
    return token_loss, mean_loss
```

```python
import functools
import math

import jax
import jax.numpy as jnp
from jax import lax
from jax.experimental import pallas as pl
from jax.experimental.pallas import tpu as pltpu
from jax.sharding import PartitionSpec as P

BLOCK = 128
SMOOTH = 0.1
CHUNK = 64
CORES = 2
F32 = jnp.float32
BF16 = jnp.bfloat16


def kernel(n, side, ndp, cap, kk, tbd, sbd, chunk, nk, c0,
           sidx, sblk, mord, msrc, mkeep, glast, ghas,
           mask_ref, t_hbm, s_hbm, w_hbm, loss_ref, mean_ref,
           tbuf, stbuf, wbuf, prob, sbuf, rb00, rb01, rb10, rb11, pscan, pown, dsnd, drcv,
           st_send, st_recv, tr, scl, smx, ftr, fsend, frecv, dsend, drecv,
           in_sem, w_sem, rs_sem, rr_sem, ds_sem, dr_sem, sts_sem, str_sem,
           fs_sem, fr_sem, es_sem, er_sem, credit, dcredit):
    half = chunk // 2
    group = CORES * side
    count = group * cap
    me = lax.axis_index("vocab")
    my_dp = lax.axis_index("dp")
    y, x, c = me // group, (me // CORES) % side, me % CORES
    rbuf = ((rb00, rb01), (rb10, rb11))
    shape = (chunk, BLOCK)
    hshape = (half, BLOCK)
    zeros = jnp.zeros(shape, F32)
    hzeros = jnp.zeros(hshape, F32)
    lane = lax.broadcasted_iota(jnp.int32, shape, 1)
    hlane = lax.broadcasted_iota(jnp.int32, hshape, 1)
    peers = [lax.rem(me + j, n) for j in range(1, n)]
    dp_peers = [lax.rem(my_dp + j, ndp) for j in range(1, ndp)]

    def dev(yy, xx, cc):
        return (yy * side + xx) * CORES + cc

    offs = [(dy, dx, dc) for dy in range(side) for dx in range(side) for dc in range(CORES)]
    offs.sort(key=lambda o: (-((o[0] > 0) + (o[1] > 0)), o[2] if o[0] or o[1] else 1 - o[2], o[0] > 0))
    slots = {}
    for h in range(2):
        for o in offs:
            if o[1 - h] or o[2]:
                slots[h, o] = len([1 for q in slots if q[0] == h])

    def parts(h, o):
        yd, xd, cd = lax.rem(y + o[0], side), lax.rem(x + o[1], side), lax.rem(c + o[2], CORES)
        if h == 0:
            return dev(y, xd, cd), yd, xd * CORES + cd
        return dev(yd, x, cd), xd, yd * CORES + cd

    mine = (x * CORES + c, y * CORES + c)

    def place(h, g, inner):
        return pl.ds((g * side + inner) * cap, cap)

    def raw_copy(par, h, o):
        j = slots[h, o]
        peer, inner, _ = parts(h, o)
        return pltpu.make_async_remote_copy(
            src_ref=sbuf.at[par, h, j], dst_ref=rbuf[par][h].at[place(h, mine[h], inner)],
            send_sem=rs_sem.at[par, h, j], recv_sem=rr_sem.at[par, h, mine[h] * side + inner],
            device_id={"vocab": peer})

    def members(h):
        out = []
        for da in range(side):
            for dc in range(CORES):
                if da or dc:
                    a = lax.rem((y if h else x) + da, side)
                    cs = lax.rem(c + dc, CORES)
                    out.append((dev(a, x, cs) if h else dev(y, a, cs), a * CORES + cs))
        return out

    def raw_wait(par, h):
        for src, g in members(h):
            for inner in range(side):
                pltpu.make_async_remote_copy(
                    src_ref=sbuf.at[par, h, 0], dst_ref=rbuf[par][h].at[place(h, g, inner)],
                    send_sem=rs_sem.at[par, h, 0], recv_sem=rr_sem.at[par, h, g * side + inner],
                    device_id={"vocab": src}).wait_recv()

    def along(h, r):
        return dev(y, lax.rem(x + r, side), c) if h else dev(lax.rem(y + r, side), x, c)

    def dense_copy(par, h, r, back=False):
        return pltpu.make_async_remote_copy(
            src_ref=dsnd.at[par, h, r - 1], dst_ref=drcv.at[par, h, r - 1],
            send_sem=ds_sem.at[par, h, r - 1], recv_sem=dr_sem.at[par, h, r - 1],
            device_id={"vocab": along(h, side - r if back else r)})

    def stat_copy(par, k, j):
        return pltpu.make_async_remote_copy(
            src_ref=st_send.at[k], dst_ref=st_recv.at[k, me],
            send_sem=sts_sem.at[par, j], recv_sem=str_sem.at[k, me],
            device_id={"vocab": peers[j]})

    def stat_wait(k, src):
        pltpu.make_async_remote_copy(
            src_ref=st_send.at[k], dst_ref=st_recv.at[k, src],
            send_sem=sts_sem.at[0, 0], recv_sem=str_sem.at[k, src],
            device_id={"vocab": src}).wait_recv()

    def cols(b):
        return pl.ds(pl.multiple_of(b * BLOCK, BLOCK), BLOCK)

    def rows(k):
        return pl.ds(pl.multiple_of(k * chunk, chunk), chunk)

    def load_t(k):
        return pltpu.make_async_copy(t_hbm.at[rows(k)], tbuf, in_sem.at[0])

    def load_s(k):
        return pltpu.make_async_copy(s_hbm.at[rows(k)], stbuf, in_sem.at[1])

    wp = math.gcd(tbd, 4)
    wn = tbd // wp * kk

    def load_w(q):
        return pltpu.make_async_copy(w_hbm.at[pl.ds(q * wn, wn)], wbuf.at[pl.ds(q * wn, wn)], w_sem.at[q])

    def bcast(column, to=shape):
        return jnp.broadcast_to(column, to)

    load_t(0).start()
    for q in range(wp):
        load_w(q).start()
    load_s(0).start()

    barrier = pltpu.get_barrier_semaphore()
    for d in peers:
        pl.semaphore_signal(barrier, inc=1, device_id={"vocab": d})
    for e in dp_peers:
        pl.semaphore_signal(barrier, inc=1, device_id={"dp": e})
    tr[...] = jnp.zeros_like(tr)
    ftr[...] = jnp.zeros_like(ftr)
    pl.semaphore_wait(barrier, n + ndp - 2)

    def scale_weights():
        for q in range(wp):
            load_w(q).wait()

            def one(b, carry):
                tiles = [wbuf[b * kk + j].astype(F32) for j in range(kk)]
                inv = 1.0 / jnp.sum(sum(tiles), axis=1, keepdims=True)
                for j in range(kk):
                    wbuf[b * kk + j] = (tiles[j] * inv).astype(BF16)
                return carry
            lax.fori_loop(q * (tbd // wp), (q + 1) * (tbd // wp), one, 0, unroll=4)

    def produce(k, par):
        load_t(k).wait()
        tmax = lax.fori_loop(
            0, tbd, lambda b, m: jnp.maximum(m, tbuf[:, cols(b)].astype(F32)),
            jnp.full(shape, -jnp.inf, F32), unroll=4)
        tmax = bcast(jnp.max(tmax, axis=1, keepdims=True))

        def expo(b, total):
            e = jnp.exp(tbuf[:, cols(b)].astype(F32) - tmax)
            prob[b] = e.astype(BF16)
            return total + e

        total = lax.fori_loop(0, tbd, expo, zeros, unroll=4)

        @pl.when(k + 1 < nk)
        def _():
            load_t(k + 1).start()

        tsum = bcast(jnp.sum(total, axis=1, keepdims=True))
        stat = jnp.where(lane == 0, tmax, jnp.where(lane == 1, tsum, 0.0))
        stat = jnp.concatenate([stat, jnp.zeros((BLOCK - chunk, BLOCK), F32)], axis=0).T[:8]
        st_send[k] = stat
        st_recv[k, me] = stat

        @pl.when(k == 0)
        def _():
            scale_weights()

        @pl.when(k >= 2)
        def _():
            for j in range(n - 1):
                stat_copy(par, k, j).wait_send()
            for h in range(2):
                for _, g in members(h):
                    pl.semaphore_wait(credit.at[h, g], 1)
        for j in range(n - 1):
            stat_copy(par, k, j).start()

        for o in offs:
            yd, xd, cd = lax.rem(y + o[0], side), lax.rem(x + o[1], side), lax.rem(c + o[2], CORES)
            d = dev(yd, xd, cd)
            dst = []
            for h in range(2):
                if (h, o) in slots:
                    @pl.when(k >= 2)
                    def _(h=h, o=o):
                        raw_copy(par, h, o).wait_send()
                    dst.append(sbuf.at[par, h, slots[h, o]])
                else:
                    dst.append(rbuf[par][h].at[place(h, mine[h], parts(h, o)[1])])

            def one(r, carry):
                i = sidx[d * cap + r]
                b = sblk[d * cap + r]
                res = jnp.dot(prob[b], wbuf[i], preferred_element_type=F32).astype(BF16)
                dst[0][r] = res[:half]
                dst[1][r] = res[half:]
                return carry
            lax.fori_loop(0, cap, one, 0, unroll=4)
            for h in range(2):
                if (h, o) in slots:
                    raw_copy(par, h, o).start()

    def merge(k, par):
        for d in peers:
            stat_wait(k, d)
        groups = (n * 8 + BLOCK - 1) // BLOCK
        per = BLOCK // 8
        columns = []
        for g in range(groups):
            for j in range(min(per, n - g * per)):
                tr[j * 8:j * 8 + 8, :] = st_recv[k, g * per + j]
            block = tr[...].T
            for j in range(min(per, n - g * per)):
                columns.append((block[:chunk, 8 * j:8 * j + 1], block[:chunk, 8 * j + 1:8 * j + 2]))
        gmax = functools.reduce(jnp.maximum, [m for m, _ in columns])
        gsum = sum(s * jnp.exp(m - gmax) for m, s in columns)
        for j, (m, _) in enumerate(columns):
            scl[j] = bcast(jnp.exp(m - gmax) / gsum)

        def scan(h, rel, dst):
            base = (h * side + rel) * count

            def step(i, acc):
                t = rbuf[par][h][mord[base + i]].astype(F32)
                acc = acc * mkeep[base + i] + t * scl[msrc[base + i], h * half:h * half + half]
                dst[i] = acc
                return acc
            lax.fori_loop(0, count, step, hzeros, unroll=4)

        for h in range(2):
            raw_wait(par, h)
            for r in range(1, side):
                scan(h, r, pscan)

                @pl.when(k >= 2)
                def _(h=h, r=r):
                    dense_copy(par, h, r).wait_send()
                base = (h * side + r) * sbd

                def pick(s, carry):
                    dsnd[par, h, r - 1, s] = (pscan[glast[base + s]] * ghas[base + s]).astype(BF16)
                    return carry
                lax.fori_loop(0, sbd, pick, 0, unroll=4)

                @pl.when(k >= 2)
                def _(h=h, r=r):
                    pl.semaphore_wait(dcredit.at[h, r - 1], 1)
                dense_copy(par, h, r).start()
        for h in range(2):
            scan(h, 0, pown.at[par, h])

            @pl.when(k + 2 < nk)
            def _(h=h):
                for src, _ in members(h):
                    pl.semaphore_signal(credit.at[h, mine[h]], inc=1, device_id={"vocab": src})

    def consume(k, par):
        load_s(k).wait()
        m = lax.fori_loop(
            0, sbd, lambda b, m: jnp.maximum(m, stbuf[:, cols(b)].astype(F32)),
            jnp.full(shape, -jnp.inf, F32), unroll=4)
        m = bcast(jnp.max(m, axis=1, keepdims=True))
        smx[...] = m
        total = lax.fori_loop(
            0, sbd, lambda b, t: t + jnp.exp(stbuf[:, cols(b)].astype(F32) - m), zeros, unroll=4)
        ssum = jnp.sum(total, axis=1, keepdims=True)
        pieces = []
        for h in range(2):
            for r in range(1, side):
                dense_copy(par, h, r, back=True).wait_recv()
            base = h * side * sbd
            top = smx[h * half:h * half + half]

            def step(s, carry):
                tot, kla = carry
                acc = pown[par, h, glast[base + s]] * ghas[base + s]
                for r in range(1, side):
                    acc = acc + drcv[par, h, r - 1, s].astype(F32)
                tgt = (1.0 - SMOOTH) * acc + c0
                z = stbuf[h * half:h * half + half, cols(s)].astype(F32) - top
                return tot + tgt, kla + tgt * (jnp.log(tgt) - z)

            tot, kla = lax.fori_loop(0, sbd, step, (hzeros,) * 2, unroll=4)
            tot, kla = [jnp.sum(v, axis=1, keepdims=True) for v in (tot, kla)]
            pieces.append(jnp.where(
                hlane == 0, kla, jnp.where(hlane == 1, tot, jnp.where(
                    hlane == 2, top, ssum[h * half:h * half + half]))))

        @pl.when(k + 1 < nk)
        def _():
            load_s(k + 1).start()

        @pl.when(k + 2 < nk)
        def _():
            for h in range(2):
                for r in range(1, side):
                    pl.semaphore_signal(dcredit.at[h, r - 1], inc=1, device_id={"vocab": along(h, side - r)})
        per = BLOCK // chunk
        ftr[pl.ds(pl.multiple_of(lax.rem(k, per) * chunk, chunk), chunk), :] = jnp.concatenate(pieces, axis=0)
        fsend[k // per] = ftr[...].T[:8]

    def pair(j, carry):
        for par in range(2):
            it = 2 * j + par

            @pl.when(it < nk)
            def _():
                produce(it, par)

            @pl.when((it >= 1) & (it <= nk))
            def _():
                merge(it - 1, 1 - par)

            @pl.when((it >= 2) & (it <= nk + 1))
            def _():
                consume(it - 2, par)
        return carry

    lax.fori_loop(0, (nk + 3) // 2, pair, 0)

    def fin_copy(d, src):
        return pltpu.make_async_remote_copy(
            src_ref=fsend, dst_ref=frecv.at[src], send_sem=fs_sem.at[d],
            recv_sem=fr_sem.at[src], device_id={"vocab": d})

    def dp_copy(e, src):
        return pltpu.make_async_remote_copy(
            src_ref=dsend, dst_ref=drecv.at[src], send_sem=es_sem.at[e],
            recv_sem=er_sem.at[src], device_id={"dp": e})

    for d in peers:
        fin_copy(d, me).start()
    frecv[me] = fsend[...]
    for d in peers:
        fin_copy(d, d).wait_recv()
    dsend[...] = jnp.zeros_like(dsend)
    for r in range(nk * chunk // BLOCK):
        parts_ = [frecv[v, r] for v in range(n)]
        gmax = functools.reduce(jnp.maximum, [p[2:3] for p in parts_])
        lse = gmax + jnp.log(sum(p[3:4] * jnp.exp(p[2:3] - gmax) for p in parts_))
        kl = sum(p[0:1] + p[1:2] * (lse - p[2:3]) for p in parts_)
        mask = mask_ref[r:r + 1, :].astype(F32)
        loss = mask * kl
        loss_ref[r:r + 1, :] = loss
        dsend[0:1, :] += loss
        dsend[1:2, :] += mask
    for e in dp_peers:
        dp_copy(e, my_dp).start()
    drecv[my_dp] = dsend[...]
    for e in dp_peers:
        dp_copy(e, e).wait_recv()
    sums = sum(drecv[v] for v in range(ndp))
    mean_ref[...] = jnp.broadcast_to(
        jnp.sum(sums[0:1], axis=1, keepdims=True) / jnp.sum(sums[1:2], axis=1, keepdims=True),
        (8, BLOCK))
    for d in peers:
        fin_copy(d, d).wait_send()
    for e in dp_peers:
        dp_copy(e, e).wait_send()
    for k in range(max(nk - 2, 0), nk):
        for j in range(n - 1):
            stat_copy(k % 2, k, j).wait_send()
        for h, o in slots:
            raw_copy(k % 2, h, o).wait_send()
        for h in range(2):
            for r in range(1, side):
                dense_copy(k % 2, h, r).wait_send()


def tables(tile_dest, n, side, cap, tbd, sbd, me):
    i32 = jnp.int32
    kk = tile_dest.shape[1]
    per = tbd * kk
    group = CORES * side
    y, x, c = me // group, (me // CORES) % side, me % CORES
    dest = tile_dest.reshape(n, per)
    owner = dest // sbd
    block = dest % sbd
    before = jnp.arange(per)[:, None] < jnp.arange(per)[None, :]
    mine = lax.dynamic_index_in_dim(owner, me, 0, keepdims=False)
    rank = jnp.sum((mine[:, None] == mine[None, :]) & before, axis=0, dtype=i32)
    slot = mine * cap + rank
    hit = slot[:, None] == jnp.arange(n * cap)[None, :]
    sidx = jnp.sum(jnp.where(hit, jnp.arange(per, dtype=i32)[:, None], 0), axis=0)

    def sources(a):
        first = lax.dynamic_slice_in_dim(a, y * group, group, 0)
        second = lax.dynamic_index_in_dim(a.reshape(side, side, CORES, per), x, 1, keepdims=False)
        return jnp.stack([first, second.reshape(group, per)])

    owns, blks = sources(owner), sources(block)
    rel = jnp.arange(side, dtype=i32)
    inner = jnp.stack([(y + rel) % side, (x + rel) % side])
    dests = jnp.stack([(inner[0] * side + x) * CORES + c, (y * side + inner[1]) * CORES + c])
    here = owns[:, None] == dests[:, :, None, None]
    rrank = jnp.sum(here[..., :, None] & before, axis=-2, dtype=i32)
    rhit = here[..., None] & (rrank[..., None] == jnp.arange(cap))
    rb = jnp.sum(jnp.where(rhit, blks[:, None, :, :, None] + 1, 0), axis=-2)
    count = group * cap
    rb = rb.reshape(2 * side, count)
    ids = jnp.arange(count, dtype=i32)
    key = jnp.where(rb > 0, rb - 1, sbd) * count + ids
    pos = jnp.sum(key[:, None, :] < key[:, :, None], axis=2, dtype=i32)
    order = jnp.sum(jnp.where(pos[:, :, None] == ids, key[:, :, None], 0), axis=1)
    blk = order // count
    o = order % count
    g = o // cap
    inner = inner.reshape(2 * side, 1)
    mord = (g * side + inner) * cap + o % cap
    along_y = jnp.arange(2 * side)[:, None] >= side
    msrc = jnp.where(along_y, (g // CORES * side + x) * CORES + g % CORES, y * group + g)
    same = blk[:, 1:] == blk[:, :-1]
    keep = jnp.concatenate([jnp.zeros((2 * side, 1), bool), same], axis=1).astype(F32)
    s = jnp.arange(sbd)[:, None]
    upto = jnp.sum(blk[:, None, :] <= s, axis=2, dtype=i32)
    has = jnp.sum(blk[:, None, :] == s, axis=2, dtype=i32) > 0
    flat = [a.reshape(-1) for a in (mord, msrc, keep, jnp.maximum(upto - 1, 0), has.astype(F32))]
    return [sidx, sidx // kk] + flat


def local(teacher_logits, student_logits, tile_dest, tile_weight, token_mask):
    n = lax.axis_size("vocab")
    ndp = lax.axis_size("dp")
    me = lax.axis_index("vocab")
    rows = teacher_logits.shape[0]
    tbd = teacher_logits.shape[1] // BLOCK
    sbd = student_logits.shape[1] // BLOCK
    kk = tile_dest.shape[1]
    cap = (tbd * kk + n - 1) // n
    side = math.isqrt(n // CORES)
    assert side * side * CORES == n and rows % BLOCK == 0
    group = CORES * side
    chunk = CHUNK
    half = chunk // 2
    nk = rows // chunk
    c0 = SMOOTH / (sbd * BLOCK * n)
    tabs = tables(tile_dest, n, side, cap, tbd, sbd, me)
    weights = tile_weight.reshape(tbd * kk, BLOCK, BLOCK)
    smem = pl.BlockSpec(memory_space=pltpu.SMEM)
    anyspec = pl.BlockSpec(memory_space=pl.ANY)
    vmem = pl.BlockSpec(memory_space=pltpu.VMEM)
    dma = pltpu.SemaphoreType.DMA
    reg = pltpu.SemaphoreType.REGULAR
    mask = token_mask.reshape(rows // BLOCK, BLOCK)
    tiles = group * side * cap
    loss, mean = pl.pallas_call(
        functools.partial(kernel, n, side, ndp, cap, kk, tbd, sbd, chunk, nk, c0),
        out_shape=[jax.ShapeDtypeStruct((rows // BLOCK, BLOCK), F32), jax.ShapeDtypeStruct((8, BLOCK), F32)],
        in_specs=[smem] * 7 + [vmem] + [anyspec] * 3,
        out_specs=[vmem] * 2,
        scratch_shapes=[
            pltpu.VMEM((chunk, tbd * BLOCK), BF16),
            pltpu.VMEM((chunk, sbd * BLOCK), BF16),
            pltpu.VMEM((tbd * kk, BLOCK, BLOCK), BF16),
            pltpu.VMEM((tbd, chunk, BLOCK), BF16),
            pltpu.VMEM((2, 2, n - side, cap, half, BLOCK), BF16)]
            + [pltpu.VMEM((tiles, half, BLOCK), BF16)] * 4 + [
            pltpu.VMEM((group * cap, half, BLOCK), F32),
            pltpu.VMEM((2, 2, group * cap, half, BLOCK), F32),
            pltpu.VMEM((2, 2, side - 1, sbd, half, BLOCK), BF16),
            pltpu.VMEM((2, 2, side - 1, sbd, half, BLOCK), BF16),
            pltpu.VMEM((nk, 8, BLOCK), F32),
            pltpu.VMEM((nk, n, 8, BLOCK), F32),
            pltpu.VMEM((BLOCK, BLOCK), F32),
            pltpu.VMEM((n, chunk, BLOCK), F32),
            pltpu.VMEM((chunk, BLOCK), F32),
            pltpu.VMEM((BLOCK, BLOCK), F32),
            pltpu.VMEM((rows // BLOCK, 8, BLOCK), F32),
            pltpu.VMEM((n, rows // BLOCK, 8, BLOCK), F32),
            pltpu.VMEM((8, BLOCK), F32),
            pltpu.VMEM((ndp, 8, BLOCK), F32),
            dma((2,)), dma((4,)),
            dma((2, 2, n - side)), dma((2, 2, group * side)),
            dma((2, 2, side - 1)), dma((2, 2, side - 1)),
            dma((2, n - 1)), dma((nk, n)),
            dma((n,)), dma((n,)), dma((ndp,)), dma((ndp,)),
            reg((2, group)), reg((2, side - 1)),
        ],
        compiler_params=pltpu.CompilerParams(
            collective_id=0, has_side_effects=True, vmem_limit_bytes=64 * 2**20 - 65536),
    )(*tabs, mask, teacher_logits, student_logits, weights)
    return loss.reshape(rows), mean[0, 0]


def solution(mesh):
    in_specs = (P("dp", "vocab"), P("dp", "vocab"), P(), P("vocab", None, None, None), P("dp"))
    out_specs = (P("dp"), P())
    return jax.shard_map(local, mesh=mesh, in_specs=in_specs, out_specs=out_specs, check_vma=False)
```

```python
import functools
import math

import jax
import jax.numpy as jnp
from jax import lax
from jax.experimental import pallas as pl
from jax.experimental.pallas import tpu as pltpu
from jax.sharding import PartitionSpec as P

BLOCK = 128
SMOOTH = 0.1
CHUNK = 64
CORES = 2
F32 = jnp.float32
BF16 = jnp.bfloat16


def build_tables(n, side, cap, kk, tbd, sbd, y, x, c, me, dest_ref, itab, ftab):
    group = CORES * side
    count = group * cap
    i32 = jnp.int32

    def iota(shape, dim):
        return lax.broadcasted_iota(i32, shape, dim)

    def add(mask, value, axis):
        return jnp.sum(jnp.where(mask, value, 0), axis=axis, keepdims=True, dtype=i32)

    def column(row):
        size = row.shape[1]
        square = (size, size)
        return add(iota(square, 0) == iota(square, 1), jnp.broadcast_to(row, square), 1)

    earlier = iota((tbd, tbd), 1) < iota((tbd, tbd), 0)

    def source(v):
        rows = [dest_ref[j, pl.ds(v, 1), :] for j in range(kk)]
        owns = [sum(jnp.where(row >= d * sbd, 1, 0) for d in range(1, n)) for row in rows]
        cols = [column(own) for own in owns]
        found = []
        for j, owner in enumerate(cols):
            same = [own == owner for own in owns[:j + 1]]
            same[j] = same[j] & earlier
            rank = jnp.sum(sum(jnp.where(m, 1, 0) for m in same), axis=1, keepdims=True, dtype=i32)
            found.append((owner, column(rows[j]) - owner * sbd, rank))
        return found

    def put(ref, r, row):
        ref[r:r + 1, :row.shape[1]] = row

    sblk = jnp.zeros((1, n * cap), i32)
    sidx = jnp.zeros((1, n * cap), i32)
    for j, (owner, _, rank) in enumerate(source(me)):
        hit = owner * cap + rank == iota((tbd, n * cap), 1)
        sblk = sblk + add(hit, iota((tbd, n * cap), 0), 0)
        sidx = sidx + add(hit, iota((tbd, n * cap), 0) * kk + j, 0)
    put(itab, 0, sidx)
    put(itab, 1, sblk)
    square = (count, count)
    before = iota(square, 1) < iota(square, 0)
    slot = iota((count, 1), 0)
    member = sum(jnp.where(slot >= g * cap, 1, 0) for g in range(1, group))
    for h in range(2):
        devs = [(g // CORES * side + x) * CORES + g % CORES if h else y * group + g for g in range(group)]
        found = [source(v) for v in devs]
        from_dev = sum(jnp.where(member == g, v, 0) for g, v in enumerate(devs))
        for rel in range(side):
            inner = lax.rem((x if h else y) + rel, side)
            d = (y * side + inner if h else inner * side + x) * CORES + c
            rb = jnp.zeros((1, count), i32)
            for g, tiles in enumerate(found):
                for owner, block, rank in tiles:
                    at = jnp.where(owner == d, rank + g * cap, -1)
                    rb = rb + add(at == iota((tbd, count), 1), block + 1, 0)
            row = jnp.where(rb > 0, rb - 1, sbd)
            col = column(row)
            again = jnp.where((row == col) & before, 1, 0)
            cont = jnp.sum(again, axis=1, keepdims=True, dtype=i32)
            pos = jnp.sum(again + jnp.where(row < col, 1, 0), axis=1, keepdims=True, dtype=i32)
            place = pos == iota(square, 1)
            base = h * side + rel
            put(itab, 2 + 3 * base, add(place, slot + member * ((side - 1) * cap) + inner * cap, 0))
            put(itab, 3 + 3 * base, add(place, from_dev, 0))
            s = iota((count, sbd), 1)
            put(itab, 4 + 3 * base, jnp.maximum(add(col <= s, 1, 0) - 1, 0))
            put(ftab, 2 * base, jnp.where(add(place, cont, 0) > 0, 1.0, 0.0))
            put(ftab, 2 * base + 1, jnp.where(add(col == s, 1, 0) > 0, 1.0, 0.0))


def kernel(n, side, ndp, cap, kk, tbd, sbd, chunk, nk, c0,
           dest_ref, mask_ref, t_hbm, s_hbm, w_hbm, loss_ref, mean_ref,
           itab, ftab, ivec, fvec, tbuf, stbuf, wbuf, prob, sbuf, rb00, rb01, rb10, rb11, pscan, pown, dsnd, drcv,
           st_send, st_recv, tr, scl, smx, tot, inv, ftr, fsend, frecv, dsend, drecv,
           in_sem, w_sem, rs_sem, rr_sem, ds_sem, dr_sem, sts_sem, str_sem,
           fs_sem, fr_sem, es_sem, er_sem, credit, dcredit):
    half = chunk // 2
    group = CORES * side
    count = group * cap
    me = lax.axis_index("vocab")
    my_dp = lax.axis_index("dp")
    y, x, c = me // group, (me // CORES) % side, me % CORES
    rbuf = ((rb00, rb01), (rb10, rb11))
    shape = (chunk, BLOCK)
    hshape = (half, BLOCK)
    zeros = jnp.zeros(shape, F32)
    hzeros = jnp.zeros(hshape, F32)
    lane = lax.broadcasted_iota(jnp.int32, shape, 1)
    hlane = lax.broadcasted_iota(jnp.int32, hshape, 1)
    peers = [lax.rem(me + j, n) for j in range(1, n)]
    dp_peers = [lax.rem(my_dp + j, ndp) for j in range(1, ndp)]

    def dev(yy, xx, cc):
        return (yy * side + xx) * CORES + cc

    offs = [(dy, dx, dc) for dy in range(side) for dx in range(side) for dc in range(CORES)]
    offs.sort(key=lambda o: (-((o[0] > 0) + (o[1] > 0)), o[2] if o[0] or o[1] else 1 - o[2], o[0] > 0))
    slots = {}
    for h in range(2):
        for o in offs:
            if o[1 - h] or o[2]:
                slots[h, o] = len([1 for q in slots if q[0] == h])

    def parts(h, o):
        yd, xd, cd = lax.rem(y + o[0], side), lax.rem(x + o[1], side), lax.rem(c + o[2], CORES)
        if h == 0:
            return dev(y, xd, cd), yd, xd * CORES + cd
        return dev(yd, x, cd), xd, yd * CORES + cd

    mine = (x * CORES + c, y * CORES + c)

    def place(h, g, inner):
        return pl.ds((g * side + inner) * cap, cap)

    def raw_copy(par, h, o):
        j = slots[h, o]
        peer, inner, _ = parts(h, o)
        return pltpu.make_async_remote_copy(
            src_ref=sbuf.at[par, h, j], dst_ref=rbuf[par][h].at[place(h, mine[h], inner)],
            send_sem=rs_sem.at[par, h, j], recv_sem=rr_sem.at[par, h, mine[h] * side + inner],
            device_id={"vocab": peer})

    def members(h):
        out = []
        for da in range(side):
            for dc in range(CORES):
                if da or dc:
                    a = lax.rem((y if h else x) + da, side)
                    cs = lax.rem(c + dc, CORES)
                    out.append((dev(a, x, cs) if h else dev(y, a, cs), a * CORES + cs))
        return out

    def raw_wait(par, h):
        for src, g in members(h):
            for inner in range(side):
                pltpu.make_async_remote_copy(
                    src_ref=sbuf.at[par, h, 0], dst_ref=rbuf[par][h].at[place(h, g, inner)],
                    send_sem=rs_sem.at[par, h, 0], recv_sem=rr_sem.at[par, h, g * side + inner],
                    device_id={"vocab": src}).wait_recv()

    def along(h, r):
        return dev(y, lax.rem(x + r, side), c) if h else dev(lax.rem(y + r, side), x, c)

    npc = math.gcd(sbd, 4)
    piece = sbd // npc

    def dense_copy(par, h, r, q, back=False):
        at = pl.ds(q * piece, piece)
        return pltpu.make_async_remote_copy(
            src_ref=dsnd.at[par, h, r - 1, at], dst_ref=drcv.at[par, h, r - 1, at],
            send_sem=ds_sem.at[par, h, r - 1, q], recv_sem=dr_sem.at[par, h, r - 1, q],
            device_id={"vocab": along(h, side - r if back else r)})

    def stat_copy(par, k, j):
        return pltpu.make_async_remote_copy(
            src_ref=st_send.at[k], dst_ref=st_recv.at[k, me],
            send_sem=sts_sem.at[par, j], recv_sem=str_sem.at[k, me],
            device_id={"vocab": peers[j]})

    def stat_wait(k, src):
        pltpu.make_async_remote_copy(
            src_ref=st_send.at[k], dst_ref=st_recv.at[k, src],
            send_sem=sts_sem.at[0, 0], recv_sem=str_sem.at[k, src],
            device_id={"vocab": src}).wait_recv()

    def cols(b):
        return pl.ds(pl.multiple_of(b * BLOCK, BLOCK), BLOCK)

    def rows(k):
        return pl.ds(pl.multiple_of(k * chunk, chunk), chunk)

    def load_t(k):
        return pltpu.make_async_copy(t_hbm.at[rows(k)], tbuf, in_sem.at[0])

    def load_s(k):
        return pltpu.make_async_copy(s_hbm.at[rows(k)], stbuf, in_sem.at[1])

    batch = math.gcd(tbd, 4)
    wp = min(4, tbd // batch)
    edges = [tbd // batch * q // wp for q in range(wp + 1)]

    def load_w(q):
        at = pl.ds(edges[q] * batch * kk, (edges[q + 1] - edges[q]) * batch * kk)
        return pltpu.make_async_copy(w_hbm.at[at], wbuf.at[at], w_sem.at[q])

    def bcast(column, to=shape):
        return jnp.broadcast_to(column, to)

    load_t(0).start()
    for q in range(wp):
        load_w(q).start()

    barrier = pltpu.get_barrier_semaphore()
    for d in peers:
        pl.semaphore_signal(barrier, inc=1, device_id={"vocab": d})
    for e in dp_peers:
        pl.semaphore_signal(barrier, inc=1, device_id={"dp": e})
    tr[...] = jnp.zeros_like(tr)
    ftr[...] = jnp.zeros_like(ftr)
    ivec[...] = jnp.zeros_like(ivec)
    fvec[...] = jnp.zeros_like(fvec)
    build_tables(n, side, cap, kk, tbd, sbd, y, x, c, me, dest_ref, ivec, fvec)
    to_smem = [pltpu.make_async_copy(ivec, itab, in_sem.at[2]), pltpu.make_async_copy(fvec, ftab, in_sem.at[3])]
    for copy in to_smem:
        copy.start()
    pl.semaphore_wait(barrier, n + ndp - 2)

    def produce(k, par):
        load_t(k).wait()

        tmax = lax.fori_loop(
            0, tbd, lambda b, m: jnp.maximum(m, tbuf[:, cols(b)].astype(F32)),
            jnp.full(shape, -jnp.inf, F32), unroll=4)
        tmax = bcast(jnp.max(tmax, axis=1, keepdims=True))

        def expo(b, total):
            e = jnp.exp(tbuf[:, cols(b)].astype(F32) - tmax)
            prob[b] = (e * inv[pl.ds(b, 1), :]).astype(BF16)
            return total + e

        @pl.when(k == 0)
        def _():
            ones = jnp.ones((kk * BLOCK, BLOCK), BF16)
            square = (BLOCK, BLOCK)
            diag = lax.broadcasted_iota(jnp.int32, square, 0) == lax.broadcasted_iota(jnp.int32, square, 1)

            def both(p, total):
                blocks = [p * batch + j for j in range(batch)]
                wide = jnp.concatenate([
                    jnp.concatenate([wbuf[b * kk + j] for j in range(kk)], axis=1) for b in blocks], axis=0)
                sums = jnp.dot(wide, ones, preferred_element_type=F32)
                for j, b in enumerate(blocks):
                    own = jnp.where(diag, sums[j * BLOCK:(j + 1) * BLOCK], 0.0)
                    inv[pl.ds(b, 1), :] = 1.0 / jnp.sum(own, axis=0, keepdims=True)
                for b in blocks:
                    total = expo(b, total)
                return total

            total = zeros
            for q in range(wp):
                load_w(q).wait()
                total = lax.fori_loop(edges[q], edges[q + 1], both, total)
            tot[...] = total
            load_s(0).start()
            for copy in to_smem:
                copy.wait()

        @pl.when(k > 0)
        def _():
            tot[...] = lax.fori_loop(0, tbd, expo, zeros, unroll=4)

        @pl.when(k + 1 < nk)
        def _():
            load_t(k + 1).start()

        tsum = bcast(jnp.sum(tot[...], axis=1, keepdims=True))
        stat = jnp.where(lane == 0, tmax, jnp.where(lane == 1, tsum, 0.0))
        stat = jnp.concatenate([stat, jnp.zeros((BLOCK - chunk, BLOCK), F32)], axis=0).T[:8]
        st_send[k] = stat
        st_recv[k, me] = stat

        @pl.when(k >= 2)
        def _():
            for j in range(n - 1):
                stat_copy(par, k, j).wait_send()
            for h in range(2):
                for _, g in members(h):
                    pl.semaphore_wait(credit.at[h, g], 1)
        for j in range(n - 1):
            stat_copy(par, k, j).start()

        for o in offs:
            yd, xd, cd = lax.rem(y + o[0], side), lax.rem(x + o[1], side), lax.rem(c + o[2], CORES)
            d = dev(yd, xd, cd)
            dst = []
            for h in range(2):
                if (h, o) in slots:
                    @pl.when(k >= 2)
                    def _(h=h, o=o):
                        raw_copy(par, h, o).wait_send()
                    dst.append(sbuf.at[par, h, slots[h, o]])
                else:
                    dst.append(rbuf[par][h].at[place(h, mine[h], parts(h, o)[1])])

            def one(r):
                i = itab[0, d * cap + r]
                b = itab[1, d * cap + r]
                res = jnp.dot(prob[b], wbuf[i], preferred_element_type=F32).astype(BF16)
                dst[0][r] = res[:half]
                dst[1][r] = res[half:]

            def several(q, carry):
                for j in range(4):
                    one(q * 4 + j)
                return carry
            lax.fori_loop(0, cap // 4, several, 0)
            for r in range(cap // 4 * 4, cap):
                one(r)
            for h in range(2):
                if (h, o) in slots:
                    raw_copy(par, h, o).start()

    def merge(k, par):
        for d in peers:
            stat_wait(k, d)
        groups = (n * 8 + BLOCK - 1) // BLOCK
        per = BLOCK // 8
        columns = []
        for g in range(groups):
            for j in range(min(per, n - g * per)):
                tr[j * 8:j * 8 + 8, :] = st_recv[k, g * per + j]
            block = tr[...].T
            for j in range(min(per, n - g * per)):
                columns.append((block[:chunk, 8 * j:8 * j + 1], block[:chunk, 8 * j + 1:8 * j + 2]))
        gmax = functools.reduce(jnp.maximum, [m for m, _ in columns])
        gsum = sum(s * jnp.exp(m - gmax) for m, s in columns)
        for j, (m, _) in enumerate(columns):
            scl[j] = bcast(jnp.exp(m - gmax) / gsum)

        def scan(h, rel, dst):
            base = 2 + 3 * (h * side + rel)
            fbase = 2 * (h * side + rel)

            def step(i, acc):
                t = rbuf[par][h][itab[base, i]].astype(F32)
                acc = acc * ftab[fbase, i] + t * scl[itab[base + 1, i], h * half:h * half + half]
                dst[i] = acc
                return acc
            lax.fori_loop(0, count, step, hzeros, unroll=4)

        for h in range(2):
            raw_wait(par, h)
            for r in range(1, side):
                scan(h, r, pscan)

                @pl.when(k >= 2)
                def _(h=h, r=r):
                    for q in range(npc):
                        dense_copy(par, h, r, q).wait_send()
                    pl.semaphore_wait(dcredit.at[h, r - 1], 1)
                base = h * side + r

                def pick(s, carry):
                    dsnd[par, h, r - 1, s] = (pscan[itab[4 + 3 * base, s]] * ftab[2 * base + 1, s]).astype(BF16)
                    return carry
                for q in range(npc):
                    lax.fori_loop(q * piece, (q + 1) * piece, pick, 0, unroll=4)
                    dense_copy(par, h, r, q).start()
        for h in range(2):
            scan(h, 0, pown.at[par, h])

            @pl.when(k + 2 < nk)
            def _(h=h):
                for src, _ in members(h):
                    pl.semaphore_signal(credit.at[h, mine[h]], inc=1, device_id={"vocab": src})

    def consume(k, par):
        load_s(k).wait()
        m = lax.fori_loop(
            0, sbd, lambda b, m: jnp.maximum(m, stbuf[:, cols(b)].astype(F32)),
            jnp.full(shape, -jnp.inf, F32), unroll=4)
        m = bcast(jnp.max(m, axis=1, keepdims=True))
        smx[...] = m
        total = lax.fori_loop(
            0, sbd, lambda b, t: t + jnp.exp(stbuf[:, cols(b)].astype(F32) - m), zeros, unroll=4)
        ssum = jnp.sum(total, axis=1, keepdims=True)
        sums = [hzeros] * 4
        for q in range(npc):
            for h in range(2):
                for r in range(1, side):
                    dense_copy(par, h, r, q, back=True).wait_recv()
                base = h * side
                top = smx[h * half:h * half + half]

                def step(s, carry):
                    tot, kla = carry
                    acc = pown[par, h, itab[4 + 3 * base, s]] * ftab[2 * base + 1, s]
                    for r in range(1, side):
                        acc = acc + drcv[par, h, r - 1, s].astype(F32)
                    tgt = (1.0 - SMOOTH) * acc + c0
                    z = stbuf[h * half:h * half + half, cols(s)].astype(F32) - top
                    return tot + tgt, kla + tgt * (jnp.log(tgt) - z)

                sums[2 * h:2 * h + 2] = lax.fori_loop(
                    q * piece, (q + 1) * piece, step, tuple(sums[2 * h:2 * h + 2]), unroll=4)
        pieces = []
        for h in range(2):
            mass, kla = [jnp.sum(v, axis=1, keepdims=True) for v in sums[2 * h:2 * h + 2]]
            pieces.append(jnp.where(
                hlane == 0, kla, jnp.where(hlane == 1, mass, jnp.where(
                    hlane == 2, smx[h * half:h * half + half], ssum[h * half:h * half + half]))))

        @pl.when(k + 1 < nk)
        def _():
            load_s(k + 1).start()

        @pl.when(k + 2 < nk)
        def _():
            for h in range(2):
                for r in range(1, side):
                    pl.semaphore_signal(dcredit.at[h, r - 1], inc=1, device_id={"vocab": along(h, side - r)})
        per = BLOCK // chunk
        ftr[pl.ds(pl.multiple_of(lax.rem(k, per) * chunk, chunk), chunk), :] = jnp.concatenate(pieces, axis=0)
        fsend[k // per] = ftr[...].T[:8]

    def pair(j, carry):
        for par in range(2):
            it = 2 * j + par

            @pl.when(it < nk)
            def _():
                produce(it, par)

            @pl.when((it >= 3) & (it <= nk + 2))
            def _():
                consume(it - 3, 1 - par)

            @pl.when((it >= 1) & (it <= nk))
            def _():
                merge(it - 1, 1 - par)
        return carry

    lax.fori_loop(0, (nk + 4) // 2, pair, 0)

    def fin_copy(d, src):
        return pltpu.make_async_remote_copy(
            src_ref=fsend, dst_ref=frecv.at[src], send_sem=fs_sem.at[d],
            recv_sem=fr_sem.at[src], device_id={"vocab": d})

    def dp_copy(e, src):
        return pltpu.make_async_remote_copy(
            src_ref=dsend, dst_ref=drecv.at[src], send_sem=es_sem.at[e],
            recv_sem=er_sem.at[src], device_id={"dp": e})

    for d in peers:
        fin_copy(d, me).start()
    frecv[me] = fsend[...]
    for d in peers:
        fin_copy(d, d).wait_recv()
    dsend[...] = jnp.zeros_like(dsend)
    for r in range(nk * chunk // BLOCK):
        parts_ = [frecv[v, r] for v in range(n)]
        gmax = functools.reduce(jnp.maximum, [p[2:3] for p in parts_])
        lse = gmax + jnp.log(sum(p[3:4] * jnp.exp(p[2:3] - gmax) for p in parts_))
        kl = sum(p[0:1] + p[1:2] * (lse - p[2:3]) for p in parts_)
        mask = mask_ref[r:r + 1, :].astype(F32)
        loss = mask * kl
        loss_ref[r:r + 1, :] = loss
        dsend[0:1, :] += loss
        dsend[1:2, :] += mask
    for e in dp_peers:
        dp_copy(e, my_dp).start()
    drecv[my_dp] = dsend[...]
    for e in dp_peers:
        dp_copy(e, e).wait_recv()
    sums = sum(drecv[v] for v in range(ndp))
    mean_ref[...] = jnp.broadcast_to(
        jnp.sum(sums[0:1], axis=1, keepdims=True) / jnp.sum(sums[1:2], axis=1, keepdims=True),
        (8, BLOCK))
    for d in peers:
        fin_copy(d, d).wait_send()
    for e in dp_peers:
        dp_copy(e, e).wait_send()
    for k in range(max(nk - 2, 0), nk):
        for j in range(n - 1):
            stat_copy(k % 2, k, j).wait_send()
        for h, o in slots:
            raw_copy(k % 2, h, o).wait_send()
        for h in range(2):
            for r in range(1, side):
                for q in range(npc):
                    dense_copy(k % 2, h, r, q).wait_send()


def local(teacher_logits, student_logits, tile_dest, tile_weight, token_mask):
    n = lax.axis_size("vocab")
    ndp = lax.axis_size("dp")
    rows = teacher_logits.shape[0]
    tbd = teacher_logits.shape[1] // BLOCK
    sbd = student_logits.shape[1] // BLOCK
    kk = tile_dest.shape[1]
    cap = (tbd * kk + n - 1) // n
    side = math.isqrt(n // CORES)
    assert side * side * CORES == n and rows % BLOCK == 0
    group = CORES * side
    chunk = CHUNK
    half = chunk // 2
    nk = rows // chunk
    c0 = SMOOTH / (sbd * BLOCK * n)
    width = -(-max(n * cap, sbd) // BLOCK) * BLOCK
    itab, ftab = (2 + 6 * side, width), (4 * side, width)
    dest = tile_dest.T.reshape(kk, n, tbd)
    weights = tile_weight.reshape(tbd * kk, BLOCK, BLOCK)
    anyspec = pl.BlockSpec(memory_space=pl.ANY)
    vmem = pl.BlockSpec(memory_space=pltpu.VMEM)
    dma = pltpu.SemaphoreType.DMA
    reg = pltpu.SemaphoreType.REGULAR
    mask = token_mask.reshape(rows // BLOCK, BLOCK)
    tiles = group * side * cap
    loss, mean = pl.pallas_call(
        functools.partial(kernel, n, side, ndp, cap, kk, tbd, sbd, chunk, nk, c0),
        out_shape=[jax.ShapeDtypeStruct((rows // BLOCK, BLOCK), F32), jax.ShapeDtypeStruct((8, BLOCK), F32)],
        in_specs=[vmem] * 2 + [anyspec] * 3,
        out_specs=[vmem] * 2,
        scratch_shapes=[
            pltpu.SMEM(itab, jnp.int32), pltpu.SMEM(ftab, F32),
            pltpu.VMEM(itab, jnp.int32), pltpu.VMEM(ftab, F32),
            pltpu.VMEM((chunk, tbd * BLOCK), BF16),
            pltpu.VMEM((chunk, sbd * BLOCK), BF16),
            pltpu.VMEM((tbd * kk, BLOCK, BLOCK), BF16),
            pltpu.VMEM((tbd, chunk, BLOCK), BF16),
            pltpu.VMEM((2, 2, n - side, cap, half, BLOCK), BF16)]
            + [pltpu.VMEM((tiles, half, BLOCK), BF16)] * 4 + [
            pltpu.VMEM((group * cap, half, BLOCK), F32),
            pltpu.VMEM((2, 2, group * cap, half, BLOCK), F32),
            pltpu.VMEM((2, 2, side - 1, sbd, half, BLOCK), BF16),
            pltpu.VMEM((2, 2, side - 1, sbd, half, BLOCK), BF16),
            pltpu.VMEM((nk, 8, BLOCK), F32),
            pltpu.VMEM((nk, n, 8, BLOCK), F32),
            pltpu.VMEM((BLOCK, BLOCK), F32),
            pltpu.VMEM((n, chunk, BLOCK), F32),
            pltpu.VMEM((chunk, BLOCK), F32),
            pltpu.VMEM((chunk, BLOCK), F32),
            pltpu.VMEM((tbd, BLOCK), F32),
            pltpu.VMEM((BLOCK, BLOCK), F32),
            pltpu.VMEM((rows // BLOCK, 8, BLOCK), F32),
            pltpu.VMEM((n, rows // BLOCK, 8, BLOCK), F32),
            pltpu.VMEM((8, BLOCK), F32),
            pltpu.VMEM((ndp, 8, BLOCK), F32),
            dma((4,)), dma((4,)),
            dma((2, 2, n - side)), dma((2, 2, group * side)),
            dma((2, 2, side - 1, 4)), dma((2, 2, side - 1, 4)),
            dma((2, n - 1)), dma((nk, n)),
            dma((n,)), dma((n,)), dma((ndp,)), dma((ndp,)),
            reg((2, group)), reg((2, side - 1)),
        ],
        compiler_params=pltpu.CompilerParams(
            collective_id=0, has_side_effects=True, vmem_limit_bytes=64 * 2**20 - 65536),
    )(dest, mask, teacher_logits, student_logits, weights)
    return loss.reshape(rows), mean[0, 0]


def solution(mesh):
    in_specs = (P("dp", "vocab"), P("dp", "vocab"), P(), P("vocab", None, None, None), P("dp"))
    out_specs = (P("dp"), P())
    return jax.shard_map(local, mesh=mesh, in_specs=in_specs, out_specs=out_specs, check_vma=False)
```

```python
import functools
import math

import jax
import jax.numpy as jnp
from jax import lax
from jax.experimental import pallas as pl
from jax.experimental.pallas import tpu as pltpu
from jax.sharding import PartitionSpec as P

BLOCK = 128
SMOOTH = 0.1
CHUNK = 64
CORES = 2
F32 = jnp.float32
BF16 = jnp.bfloat16


def table_tools(n, kk, tbd, sbd, dest_ref):
    i32 = jnp.int32

    def iota(shape, dim):
        return lax.broadcasted_iota(i32, shape, dim)

    def add(mask, value, axis):
        return jnp.sum(jnp.where(mask, value, 0), axis=axis, keepdims=True, dtype=i32)

    def column(row):
        size = row.shape[1]
        square = (size, size)
        return add(iota(square, 0) == iota(square, 1), jnp.broadcast_to(row, square), 1)

    earlier = iota((tbd, tbd), 1) < iota((tbd, tbd), 0)

    def source(v):
        wide = (tbd, dest_ref.shape[1])
        here = iota(wide, 1) == iota(wide, 0) + v * tbd
        dests = [add(here, jnp.broadcast_to(dest_ref[j:j + 1, :], wide), 1) for j in range(kk)]
        diag = iota((tbd, tbd), 0) == iota((tbd, tbd), 1)
        rows = [add(diag, jnp.broadcast_to(d, (tbd, tbd)), 0) for d in dests]
        owns = [sum(jnp.where(row >= d * sbd, 1, 0) for d in range(1, n)) for row in rows]
        cols = [sum(jnp.where(d >= e * sbd, 1, 0) for e in range(1, n)) for d in dests]
        found = []
        for j, owner in enumerate(cols):
            same = [own == owner for own in owns[:j + 1]]
            same[j] = same[j] & earlier
            rank = jnp.sum(sum(jnp.where(m, 1, 0) for m in same), axis=1, keepdims=True, dtype=i32)
            found.append((owner, dests[j] - owner * sbd, rank))
        return found

    def put(ref, r, row):
        ref[r:r + 1, :row.shape[1]] = row

    return iota, add, column, source, put


def send_table(n, cap, kk, tbd, sbd, me, dest_ref, stab):
    i32 = jnp.int32
    iota, add, column, source, put = table_tools(n, kk, tbd, sbd, dest_ref)
    sblk = jnp.zeros((1, n * cap), i32)
    sidx = jnp.zeros((1, n * cap), i32)
    for j, (owner, _, rank) in enumerate(source(me)):
        hit = owner * cap + rank == iota((tbd, n * cap), 1)
        sblk = sblk + add(hit, iota((tbd, n * cap), 0), 0)
        sidx = sidx + add(hit, iota((tbd, n * cap), 0) * kk + j, 0)
    put(stab, 0, sidx)
    put(stab, 1, sblk)


def receive_tables(n, side, cap, kk, tbd, sbd, y, x, c, dest_ref, itab, ftab):
    i32 = jnp.int32
    group = CORES * side
    count = group * cap
    iota, add, column, source, put = table_tools(n, kk, tbd, sbd, dest_ref)
    square = (count, count)
    before = iota(square, 1) < iota(square, 0)
    slot = iota((count, 1), 0)
    member = sum(jnp.where(slot >= g * cap, 1, 0) for g in range(1, group))
    for h in range(2):
        devs = [(g // CORES * side + x) * CORES + g % CORES if h else y * group + g for g in range(group)]
        found = [source(v) for v in devs]
        from_dev = sum(jnp.where(member == g, v, 0) for g, v in enumerate(devs))
        for rel in range(side):
            inner = lax.rem((x if h else y) + rel, side)
            d = (y * side + inner if h else inner * side + x) * CORES + c
            rb = jnp.zeros((1, count), i32)
            for g, tiles in enumerate(found):
                for owner, block, rank in tiles:
                    at = jnp.where(owner == d, rank + g * cap, -1)
                    rb = rb + add(at == iota((tbd, count), 1), block + 1, 0)
            row = jnp.where(rb > 0, rb - 1, sbd)
            col = column(row)
            again = jnp.where((row == col) & before, 1, 0)
            cont = jnp.sum(again, axis=1, keepdims=True, dtype=i32)
            pos = jnp.sum(again + jnp.where(row < col, 1, 0), axis=1, keepdims=True, dtype=i32)
            place = pos == iota(square, 1)
            base = h * side + rel
            put(itab, 3 * base, add(place, slot + member * ((side - 1) * cap) + inner * cap, 0))
            put(itab, 1 + 3 * base, add(place, from_dev, 0))
            s = iota((count, sbd), 1)
            put(itab, 2 + 3 * base, jnp.maximum(add(col <= s, 1, 0) - 1, 0))
            put(ftab, 2 * base, jnp.where(add(place, cont, 0) > 0, 1.0, 0.0))
            put(ftab, 2 * base + 1, jnp.where(add(col == s, 1, 0) > 0, 1.0, 0.0))


def kernel(n, side, ndp, cap, kk, tbd, sbd, chunk, nk, c0,
           dest_ref, mask_ref, t_hbm, s_hbm, w_hbm, loss_ref, mean_ref,
           stab, itab, ftab, svec, ivec, fvec, tbuf, stbuf, wbuf, prob, sbuf, rb00, rb01, rb10, rb11, pscan, pown, dsnd, drcv,
           st_send, st_recv, tr, scl, smx, inv, ftr, fsend, frecv, dsend, drecv,
           in_sem, w_sem, rs_sem, rr_sem, ds_sem, dr_sem, sts_sem, str_sem,
           fs_sem, fr_sem, es_sem, er_sem, credit, dcredit):
    half = chunk // 2
    group = CORES * side
    count = group * cap
    me = lax.axis_index("vocab")
    my_dp = lax.axis_index("dp")
    y, x, c = me // group, (me // CORES) % side, me % CORES
    rbuf = ((rb00, rb01), (rb10, rb11))
    shape = (chunk, BLOCK)
    hshape = (half, BLOCK)
    zeros = jnp.zeros(shape, F32)
    hzeros = jnp.zeros(hshape, F32)
    lane = lax.broadcasted_iota(jnp.int32, shape, 1)
    hlane = lax.broadcasted_iota(jnp.int32, hshape, 1)
    peers = [lax.rem(me + j, n) for j in range(1, n)]
    dp_peers = [lax.rem(my_dp + j, ndp) for j in range(1, ndp)]

    def dev(yy, xx, cc):
        return (yy * side + xx) * CORES + cc

    offs = [(dy, dx, dc) for dy in range(side) for dx in range(side) for dc in range(CORES)]
    offs.sort(key=lambda o: (-((o[0] > 0) + (o[1] > 0)), o[2] if o[0] or o[1] else 1 - o[2], o[0] > 0))
    slots = {}
    for h in range(2):
        for o in offs:
            if o[1 - h] or o[2]:
                slots[h, o] = len([1 for q in slots if q[0] == h])

    def parts(h, o):
        yd, xd, cd = lax.rem(y + o[0], side), lax.rem(x + o[1], side), lax.rem(c + o[2], CORES)
        if h == 0:
            return dev(y, xd, cd), yd, xd * CORES + cd
        return dev(yd, x, cd), xd, yd * CORES + cd

    mine = (x * CORES + c, y * CORES + c)

    def place(h, g, inner):
        return pl.ds((g * side + inner) * cap, cap)

    def raw_copy(par, h, o):
        j = slots[h, o]
        peer, inner, _ = parts(h, o)
        return pltpu.make_async_remote_copy(
            src_ref=sbuf.at[par, h, j], dst_ref=rbuf[par][h].at[place(h, mine[h], inner)],
            send_sem=rs_sem.at[par, h, j], recv_sem=rr_sem.at[par, h, mine[h] * side + inner],
            device_id={"vocab": peer})

    def members(h):
        out = []
        for da in range(side):
            for dc in range(CORES):
                if da or dc:
                    a = lax.rem((y if h else x) + da, side)
                    cs = lax.rem(c + dc, CORES)
                    out.append((dev(a, x, cs) if h else dev(y, a, cs), a * CORES + cs))
        return out

    def raw_wait(par, h):
        for src, g in members(h):
            for inner in range(side):
                pltpu.make_async_remote_copy(
                    src_ref=sbuf.at[par, h, 0], dst_ref=rbuf[par][h].at[place(h, g, inner)],
                    send_sem=rs_sem.at[par, h, 0], recv_sem=rr_sem.at[par, h, g * side + inner],
                    device_id={"vocab": src}).wait_recv()

    def along(h, r):
        return dev(y, lax.rem(x + r, side), c) if h else dev(lax.rem(y + r, side), x, c)

    npc = math.gcd(sbd, 4)
    piece = sbd // npc

    def dense_copy(par, h, r, q, back=False):
        at = pl.ds(q * piece, piece)
        return pltpu.make_async_remote_copy(
            src_ref=dsnd.at[par, h, r - 1, at], dst_ref=drcv.at[par, h, r - 1, at],
            send_sem=ds_sem.at[par, h, r - 1, q], recv_sem=dr_sem.at[par, h, r - 1, q],
            device_id={"vocab": along(h, side - r if back else r)})

    def stat_copy(par, k, j):
        return pltpu.make_async_remote_copy(
            src_ref=st_send.at[k], dst_ref=st_recv.at[k, me],
            send_sem=sts_sem.at[par, j], recv_sem=str_sem.at[k, me],
            device_id={"vocab": peers[j]})

    def stat_wait(k, src):
        pltpu.make_async_remote_copy(
            src_ref=st_send.at[k], dst_ref=st_recv.at[k, src],
            send_sem=sts_sem.at[0, 0], recv_sem=str_sem.at[k, src],
            device_id={"vocab": src}).wait_recv()

    def fin_copy(r, d, src):
        return pltpu.make_async_remote_copy(
            src_ref=fsend.at[r], dst_ref=frecv.at[src, r], send_sem=fs_sem.at[r, d],
            recv_sem=fr_sem.at[r, src], device_id={"vocab": d})

    def cols(b):
        return pl.ds(pl.multiple_of(b * BLOCK, BLOCK), BLOCK)

    def rows(k):
        return pl.ds(pl.multiple_of(k * chunk, chunk), chunk)

    def load_t(k):
        return pltpu.make_async_copy(t_hbm.at[rows(k)], tbuf, in_sem.at[0])

    def load_s(k):
        return pltpu.make_async_copy(s_hbm.at[rows(k)], stbuf, in_sem.at[1])

    batch = math.gcd(tbd, 4)
    wp = min(4, tbd // batch)
    edges = [tbd // batch * q // wp for q in range(wp + 1)]

    def load_w(q):
        at = pl.ds(edges[q] * batch * kk, (edges[q + 1] - edges[q]) * batch * kk)
        return pltpu.make_async_copy(w_hbm.at[at], wbuf.at[at], w_sem.at[q])

    def bcast(column, to=shape):
        return jnp.broadcast_to(column, to)

    for q in range(wp):
        load_w(q).start()
    load_t(0).start()

    barrier = pltpu.get_barrier_semaphore()
    for d in peers:
        pl.semaphore_signal(barrier, inc=1, device_id={"vocab": d})
    for e in dp_peers:
        pl.semaphore_signal(barrier, inc=1, device_id={"dp": e})
    tr[...] = jnp.zeros_like(tr)
    ftr[...] = jnp.zeros_like(ftr)
    svec[...] = jnp.zeros_like(svec)
    ivec[...] = jnp.zeros_like(ivec)
    fvec[...] = jnp.zeros_like(fvec)
    send_table(n, cap, kk, tbd, sbd, me, dest_ref, svec)
    send_copy = pltpu.make_async_copy(svec, stab, in_sem.at[2])
    send_copy.start()
    receive_copies = [pltpu.make_async_copy(ivec, itab, in_sem.at[3]), pltpu.make_async_copy(fvec, ftab, in_sem.at[4])]

    def weight_sums(p, carry):
        for j in range(batch):
            b = p * batch + j
            whole = sum(wbuf[b * kk + i].astype(F32) for i in range(kk))
            inv[pl.ds(b, 1), :] = 1.0 / jnp.sum(whole.T, axis=0, keepdims=True)
        return carry

    for q in range(wp):
        load_w(q).wait()
        lax.fori_loop(edges[q], edges[q + 1], weight_sums, 0)
    send_copy.wait()
    pl.semaphore_wait(barrier, n + ndp - 2)

    def produce(k, par):
        load_t(k).wait()

        tmax = lax.fori_loop(
            0, tbd, lambda b, m: jnp.maximum(m, tbuf[:, cols(b)].astype(F32)),
            jnp.full(shape, -jnp.inf, F32), unroll=4)
        tmax = bcast(jnp.max(tmax, axis=1, keepdims=True))

        def expo(b, total):
            e = jnp.exp(tbuf[:, cols(b)].astype(F32) - tmax)
            prob[b] = (e * inv[pl.ds(b, 1), :]).astype(BF16)
            return total + e

        total = lax.fori_loop(0, tbd, expo, zeros, unroll=4)

        @pl.when(k + 1 < nk)
        def _():
            load_t(k + 1).start()

        tsum = bcast(jnp.sum(total, axis=1, keepdims=True))
        stat = jnp.where(lane == 0, tmax, jnp.where(lane == 1, tsum, 0.0))
        stat = jnp.concatenate([stat, jnp.zeros((BLOCK - chunk, BLOCK), F32)], axis=0).T[:2]
        st_send[k] = stat
        st_recv[k, me] = stat

        @pl.when(k >= 2)
        def _():
            for j in range(n - 1):
                stat_copy(par, k, j).wait_send()
            for h in range(2):
                for _, g in members(h):
                    pl.semaphore_wait(credit.at[h, g], 1)
        for j in range(n - 1):
            stat_copy(par, k, j).start()

        for o in offs:
            yd, xd, cd = lax.rem(y + o[0], side), lax.rem(x + o[1], side), lax.rem(c + o[2], CORES)
            d = dev(yd, xd, cd)
            dst = []
            for h in range(2):
                if (h, o) in slots:
                    @pl.when(k >= 2)
                    def _(h=h, o=o):
                        raw_copy(par, h, o).wait_send()
                    dst.append(sbuf.at[par, h, slots[h, o]])
                else:
                    dst.append(rbuf[par][h].at[place(h, mine[h], parts(h, o)[1])])

            def one(r):
                i = stab[0, d * cap + r]
                b = stab[1, d * cap + r]
                res = jnp.dot(prob[b], wbuf[i], preferred_element_type=F32).astype(BF16)
                dst[0][r] = res[:half]
                dst[1][r] = res[half:]

            def several(q, carry):
                for j in range(4):
                    one(q * 4 + j)
                return carry
            lax.fori_loop(0, cap // 4, several, 0)
            for r in range(cap // 4 * 4, cap):
                one(r)
            for h in range(2):
                if (h, o) in slots:
                    raw_copy(par, h, o).start()

    def merge(k, par):
        for d in peers:
            stat_wait(k, d)
        groups = (n * 8 + BLOCK - 1) // BLOCK
        per = BLOCK // 8
        columns = []
        for g in range(groups):
            for j in range(min(per, n - g * per)):
                tr[j * 8:j * 8 + 2, :] = st_recv[k, g * per + j]
            block = tr[...].T
            for j in range(min(per, n - g * per)):
                columns.append((block[:chunk, 8 * j:8 * j + 1], block[:chunk, 8 * j + 1:8 * j + 2]))
        gmax = functools.reduce(jnp.maximum, [m for m, _ in columns])
        gsum = sum(s * jnp.exp(m - gmax) for m, s in columns)
        for j, (m, _) in enumerate(columns):
            scl[j] = bcast(jnp.exp(m - gmax) / gsum)

        def scan(h, rel, dst):
            base = 3 * (h * side + rel)
            fbase = 2 * (h * side + rel)

            def step(i, acc):
                t = rbuf[par][h][itab[base, i]].astype(F32)
                acc = acc * ftab[fbase, i] + t * scl[itab[base + 1, i], h * half:h * half + half]
                dst[i] = acc
                return acc
            lax.fori_loop(0, count, step, hzeros, unroll=4)

        for h in range(2):
            raw_wait(par, h)
            for r in range(1, side):
                scan(h, r, pscan)

                @pl.when(k >= 2)
                def _(h=h, r=r):
                    for q in range(npc):
                        dense_copy(par, h, r, q).wait_send()
                    pl.semaphore_wait(dcredit.at[h, r - 1], 1)
                base = h * side + r

                def pick(s, carry):
                    dsnd[par, h, r - 1, s] = (pscan[itab[2 + 3 * base, s]] * ftab[2 * base + 1, s]).astype(BF16)
                    return carry
                for q in range(npc):
                    lax.fori_loop(q * piece, (q + 1) * piece, pick, 0, unroll=4)
                    dense_copy(par, h, r, q).start()
        for h in range(2):
            scan(h, 0, pown.at[par, h])

            @pl.when(k + 2 < nk)
            def _(h=h):
                for src, _ in members(h):
                    pl.semaphore_signal(credit.at[h, mine[h]], inc=1, device_id={"vocab": src})

    def consume(k, par):
        load_s(k).wait()
        m = lax.fori_loop(
            0, sbd, lambda b, m: jnp.maximum(m, stbuf[:, cols(b)].astype(F32)),
            jnp.full(shape, -jnp.inf, F32), unroll=4)
        m = bcast(jnp.max(m, axis=1, keepdims=True))
        smx[...] = m
        total = lax.fori_loop(
            0, sbd, lambda b, t: t + jnp.exp(stbuf[:, cols(b)].astype(F32) - m), zeros, unroll=4)
        ssum = jnp.sum(total, axis=1, keepdims=True)
        sums = [hzeros] * 4
        for q in range(npc):
            for h in range(2):
                for r in range(1, side):
                    dense_copy(par, h, r, q, back=True).wait_recv()
                base = h * side
                top = smx[h * half:h * half + half]

                def step(s, carry):
                    tot, kla = carry
                    acc = pown[par, h, itab[2 + 3 * base, s]] * ftab[2 * base + 1, s]
                    for r in range(1, side):
                        acc = acc + drcv[par, h, r - 1, s].astype(F32)
                    tgt = (1.0 - SMOOTH) * acc + c0
                    z = stbuf[h * half:h * half + half, cols(s)].astype(F32) - top
                    return tot + tgt, kla + tgt * (jnp.log(tgt) - z)

                sums[2 * h:2 * h + 2] = lax.fori_loop(
                    q * piece, (q + 1) * piece, step, tuple(sums[2 * h:2 * h + 2]), unroll=4)
        pieces = []
        for h in range(2):
            mass, kla = [jnp.sum(v, axis=1, keepdims=True) for v in sums[2 * h:2 * h + 2]]
            pieces.append(jnp.where(
                hlane == 0, kla, jnp.where(hlane == 1, mass, jnp.where(
                    hlane == 2, smx[h * half:h * half + half], ssum[h * half:h * half + half]))))

        @pl.when(k + 1 < nk)
        def _():
            load_s(k + 1).start()

        @pl.when(k + 2 < nk)
        def _():
            for h in range(2):
                for r in range(1, side):
                    pl.semaphore_signal(dcredit.at[h, r - 1], inc=1, device_id={"vocab": along(h, side - r)})
        per = BLOCK // chunk
        ftr[pl.ds(pl.multiple_of(lax.rem(k, per) * chunk, chunk), chunk), :] = jnp.concatenate(pieces, axis=0)

        @pl.when(lax.rem(k, per) == per - 1)
        def _():
            r = k // per
            fsend[r] = ftr[...].T[:4]
            for j in range(n - 1):
                fin_copy(r, peers[j], me).start()

    def pair(j, carry):
        for par in range(2):
            it = 2 * j + par

            @pl.when(it < nk)
            def _():
                produce(it, par)

            if par == 0:
                @pl.when(it == 0)
                def _():
                    load_s(0).start()
                    receive_tables(n, side, cap, kk, tbd, sbd, y, x, c, dest_ref, ivec, fvec)
                    for copy in receive_copies:
                        copy.start()
                    for copy in receive_copies:
                        copy.wait()

            @pl.when((it >= 3) & (it <= nk + 2))
            def _():
                consume(it - 3, 1 - par)

            @pl.when((it >= 1) & (it <= nk))
            def _():
                merge(it - 1, 1 - par)
        return carry

    lax.fori_loop(0, (nk + 4) // 2, pair, 0)

    def dp_copy(e, src):
        return pltpu.make_async_remote_copy(
            src_ref=dsend, dst_ref=drecv.at[src], send_sem=es_sem.at[e],
            recv_sem=er_sem.at[src], device_id={"dp": e})

    frecv[me] = fsend[...]
    dsend[...] = jnp.zeros_like(dsend)
    for r in range(nk * chunk // BLOCK):
        for d in peers:
            fin_copy(r, d, d).wait_recv()
        parts_ = [frecv[v, r] for v in range(n)]
        gmax = functools.reduce(jnp.maximum, [p[2:3] for p in parts_])
        lse = gmax + jnp.log(sum(p[3:4] * jnp.exp(p[2:3] - gmax) for p in parts_))
        kl = sum(p[0:1] + p[1:2] * (lse - p[2:3]) for p in parts_)
        mask = mask_ref[r:r + 1, :].astype(F32)
        loss = mask * kl
        loss_ref[r:r + 1, :] = loss
        dsend[0:1, :] += loss
        dsend[1:2, :] += mask
    for e in dp_peers:
        dp_copy(e, my_dp).start()
    drecv[my_dp] = dsend[...]
    for e in dp_peers:
        dp_copy(e, e).wait_recv()
    sums = sum(drecv[v] for v in range(ndp))
    mean_ref[...] = jnp.broadcast_to(
        jnp.sum(sums[0:1], axis=1, keepdims=True) / jnp.sum(sums[1:2], axis=1, keepdims=True),
        (8, BLOCK))
    for r in range(nk * chunk // BLOCK):
        for d in peers:
            fin_copy(r, d, d).wait_send()
    for e in dp_peers:
        dp_copy(e, e).wait_send()
    for k in range(max(nk - 2, 0), nk):
        for j in range(n - 1):
            stat_copy(k % 2, k, j).wait_send()
        for h, o in slots:
            raw_copy(k % 2, h, o).wait_send()
        for h in range(2):
            for r in range(1, side):
                for q in range(npc):
                    dense_copy(k % 2, h, r, q).wait_send()


def local(teacher_logits, student_logits, tile_dest, tile_weight, token_mask):
    n = lax.axis_size("vocab")
    ndp = lax.axis_size("dp")
    rows = teacher_logits.shape[0]
    tbd = teacher_logits.shape[1] // BLOCK
    sbd = student_logits.shape[1] // BLOCK
    kk = tile_dest.shape[1]
    cap = (tbd * kk + n - 1) // n
    side = math.isqrt(n // CORES)
    assert side * side * CORES == n and rows % BLOCK == 0
    group = CORES * side
    chunk = CHUNK
    half = chunk // 2
    nk = rows // chunk
    c0 = SMOOTH / (sbd * BLOCK * n)
    width = -(-max(n * cap, sbd) // BLOCK) * BLOCK
    stab, itab, ftab = (2, width), (6 * side, width), (4 * side, width)
    dest = tile_dest.T
    weights = tile_weight.reshape(tbd * kk, BLOCK, BLOCK)
    anyspec = pl.BlockSpec(memory_space=pl.ANY)
    vmem = pl.BlockSpec(memory_space=pltpu.VMEM)
    dma = pltpu.SemaphoreType.DMA
    reg = pltpu.SemaphoreType.REGULAR
    mask = token_mask.reshape(rows // BLOCK, BLOCK)
    tiles = group * side * cap
    loss, mean = pl.pallas_call(
        functools.partial(kernel, n, side, ndp, cap, kk, tbd, sbd, chunk, nk, c0),
        out_shape=[jax.ShapeDtypeStruct((rows // BLOCK, BLOCK), F32), jax.ShapeDtypeStruct((8, BLOCK), F32)],
        in_specs=[vmem] * 2 + [anyspec] * 3,
        out_specs=[vmem] * 2,
        scratch_shapes=[
            pltpu.SMEM(stab, jnp.int32), pltpu.SMEM(itab, jnp.int32), pltpu.SMEM(ftab, F32),
            pltpu.VMEM(stab, jnp.int32), pltpu.VMEM(itab, jnp.int32), pltpu.VMEM(ftab, F32),
            pltpu.VMEM((chunk, tbd * BLOCK), BF16),
            pltpu.VMEM((chunk, sbd * BLOCK), BF16),
            pltpu.VMEM((tbd * kk, BLOCK, BLOCK), BF16),
            pltpu.VMEM((tbd, chunk, BLOCK), BF16),
            pltpu.VMEM((2, 2, n - side, cap, half, BLOCK), BF16)]
            + [pltpu.VMEM((tiles, half, BLOCK), BF16)] * 4 + [
            pltpu.VMEM((group * cap, half, BLOCK), F32),
            pltpu.VMEM((2, 2, group * cap, half, BLOCK), F32),
            pltpu.VMEM((2, 2, side - 1, sbd, half, BLOCK), BF16),
            pltpu.VMEM((2, 2, side - 1, sbd, half, BLOCK), BF16),
            pltpu.VMEM((nk, 2, BLOCK), F32),
            pltpu.VMEM((nk, n, 2, BLOCK), F32),
            pltpu.VMEM((BLOCK, BLOCK), F32),
            pltpu.VMEM((n, chunk, BLOCK), F32),
            pltpu.VMEM((chunk, BLOCK), F32),
            pltpu.VMEM((tbd, BLOCK), F32),
            pltpu.VMEM((BLOCK, BLOCK), F32),
            pltpu.VMEM((rows // BLOCK, 4, BLOCK), F32),
            pltpu.VMEM((n, rows // BLOCK, 4, BLOCK), F32),
            pltpu.VMEM((8, BLOCK), F32),
            pltpu.VMEM((ndp, 8, BLOCK), F32),
            dma((5,)), dma((4,)),
            dma((2, 2, n - side)), dma((2, 2, group * side)),
            dma((2, 2, side - 1, 4)), dma((2, 2, side - 1, 4)),
            dma((2, n - 1)), dma((nk, n)),
            dma((rows // BLOCK, n)), dma((rows // BLOCK, n)), dma((ndp,)), dma((ndp,)),
            reg((2, group)), reg((2, side - 1)),
        ],
        compiler_params=pltpu.CompilerParams(
            collective_id=0, has_side_effects=True, vmem_limit_bytes=64 * 2**20 - 65536),
    )(dest, mask, teacher_logits, student_logits, weights)
    return loss.reshape(rows), mean[0, 0]


def solution(mesh):
    in_specs = (P("dp", "vocab"), P("dp", "vocab"), P(), P("vocab", None, None, None), P("dp"))
    out_specs = (P("dp"), P())
    return jax.shard_map(local, mesh=mesh, in_specs=in_specs, out_specs=out_specs, check_vma=False)
```
